8 devices in a mesh: data: 1 (over z), dap: 8 (over y, x, core).
Axes of the slice: x: 2, y: 2, z: 1, core: 2. Of those that a mesh axis runs over, the one named last changes fastest.
Arguments:
- pair_act: float32 [512, 512, 128], P(('data', 'dap'))
- pair_mask: int32 [512, 512], P(('data', 'dap'))
- grad_out: float32 [512, 512, 128], P(('data', 'dap'))
- ln_pair: bfloat16 [2, 2, 128], replicated
- w_in: bfloat16 [2, 128, 640], replicated
- ln_tri: bfloat16 [2, 2, 128], replicated
- w_out: bfloat16 [2, 128, 128], replicated
Outputs:
- output 1: float32 [512, 512, 128], P(('data', 'dap'))
- output 2: float32 [2, 2, 128], P('data')
- output 3: float32 [2, 128, 640], P('data')
- output 4: float32 [2, 2, 128], P('data')
- output 5: float32 [2, 128, 128], P('data')
All inputs are finite; a program needn't handle non-finite values.
Results may differ from the reference program's by a relative error of at most 0.0135825.
Values are sent between devices in bfloat16 or wider.
A program may use at most 1 GiB of HBM per device.

```python
import jax
import jax.numpy as jnp
from jax import lax

PAIR_DIM = 128
HIDDEN = 128
ROWS_DEV = 64
GROUP_SIZE = 8
SEQ_LEN = ROWS_DEV * GROUP_SIZE
LN_EPS = 1e-5
OUT_FORM = 'ikc,jkc->ijc'
IN_FORM = 'kic,kjc->ijc'


def setup_inputs(seed: int = 0, part: int = 0) -> dict:
    part_keys = jax.random.split(jax.random.fold_in(jax.random.key(seed), part), 3)
    shared_keys = jax.random.split(jax.random.key(seed + 1), 6)
    width_in = 4 * HIDDEN + PAIR_DIM
    pair_act = jax.random.normal(part_keys[0], (SEQ_LEN, SEQ_LEN, PAIR_DIM), jnp.float32)
    tail_len = jax.random.randint(part_keys[1], (), SEQ_LEN // 16 + 1, SEQ_LEN // 8 + 2)
    seq_mask = (jnp.arange(SEQ_LEN) < SEQ_LEN - tail_len).astype(jnp.int32)
    pair_mask = seq_mask[:, None] * seq_mask[None, :]
    grad_out = jax.random.normal(part_keys[2], (SEQ_LEN, SEQ_LEN, PAIR_DIM), jnp.float32)
    gain_pair = 1.0 + 0.3 * jax.random.normal(shared_keys[0], (2, 1, PAIR_DIM), jnp.float32)
    bias_pair = 0.3 * jax.random.normal(shared_keys[1], (2, 1, PAIR_DIM), jnp.float32)
    w_in = jax.random.normal(shared_keys[2], (2, PAIR_DIM, width_in), jnp.float32) * PAIR_DIM ** -0.5
    gain_tri = 1.0 + 0.3 * jax.random.normal(shared_keys[3], (2, 1, HIDDEN), jnp.float32)
    bias_tri = 0.3 * jax.random.normal(shared_keys[4], (2, 1, HIDDEN), jnp.float32)
    w_out = jax.random.normal(shared_keys[5], (2, HIDDEN, PAIR_DIM), jnp.float32) * HIDDEN ** -0.5
    return {
        'pair_act': pair_act,
        'pair_mask': pair_mask,
        'grad_out': grad_out,
        'ln_pair': jnp.concatenate([gain_pair, bias_pair], axis=1).astype(jnp.bfloat16),
        'w_in': w_in.astype(jnp.bfloat16),
        'ln_tri': jnp.concatenate([gain_tri, bias_tri], axis=1).astype(jnp.bfloat16),
        'w_out': w_out.astype(jnp.bfloat16),
    }


def layer_norm(values, gain_vec, bias_vec):
    mean_val = jnp.mean(values, axis=-1, keepdims=True)
    centred = values - mean_val
    variance = jnp.mean(centred * centred, axis=-1, keepdims=True)
    return centred * lax.rsqrt(variance + LN_EPS) * gain_vec + bias_vec


def project_rows(row_vals, mask_rows, ln_pair, w_in):
    normed = layer_norm(row_vals, ln_pair[0], ln_pair[1]).astype(jnp.bfloat16)
    proj_all = jnp.einsum('ijc,cd->ijd', normed.astype(jnp.float32), w_in)
    mask_f = mask_rows.astype(jnp.float32)[:, :, None]
    left_act = (mask_f * jax.nn.sigmoid(proj_all[:, :, HIDDEN:2 * HIDDEN]) * proj_all[:, :, :HIDDEN]).astype(jnp.bfloat16)
    right_act = (mask_f * jax.nn.sigmoid(proj_all[:, :, 3 * HIDDEN:4 * HIDDEN]) * proj_all[:, :, 2 * HIDDEN:3 * HIDDEN]).astype(jnp.bfloat16)
    gate_act = jax.nn.sigmoid(proj_all[:, :, 4 * HIDDEN:])
    return left_act, right_act, gate_act


def finish_rows(row_vals, tri_sum, gate_act, ln_tri, w_out):
    tri_norm = layer_norm(tri_sum, ln_tri[0], ln_tri[1]).astype(jnp.bfloat16)
    return row_vals + gate_act * jnp.einsum('ijc,cd->ijd', tri_norm.astype(jnp.float32), w_out)


def tri_update(pair_act, pair_mask, ln_pair, w_in, ln_tri, w_out, ein_form):
    block_shape = (GROUP_SIZE, ROWS_DEV, SEQ_LEN)
    pair_blocks = pair_act.reshape(block_shape + (PAIR_DIM,))
    left_act, right_act, gate_act = lax.map(
        jax.checkpoint(lambda row_block: project_rows(row_block[0], row_block[1], ln_pair, w_in)),
        (pair_blocks, pair_mask.reshape(block_shape)))
    tri_sum = jnp.einsum(ein_form,
                         left_act.reshape(SEQ_LEN, SEQ_LEN, HIDDEN).astype(jnp.float32),
                         right_act.reshape(SEQ_LEN, SEQ_LEN, HIDDEN).astype(jnp.float32))
    new_blocks = lax.map(
        jax.checkpoint(lambda row_block: finish_rows(row_block[0], row_block[1], row_block[2], ln_tri, w_out)),
        (pair_blocks, tri_sum.reshape(block_shape + (HIDDEN,)), gate_act))
    return new_blocks.reshape(SEQ_LEN, SEQ_LEN, PAIR_DIM)


def block_forward(pair_act, pair_mask, ln_pair, w_in, ln_tri, w_out):
    mid_act = tri_update(pair_act, pair_mask, ln_pair[0], w_in[0], ln_tri[0], w_out[0], OUT_FORM)
    return tri_update(mid_act, pair_mask, ln_pair[1], w_in[1], ln_tri[1], w_out[1], IN_FORM)


def reference(pair_act, pair_mask, grad_out, ln_pair, w_in, ln_tri, w_out):
    def forward(pair_in, ln_pair_v, w_in_v, ln_tri_v, w_out_v):
        return block_forward(pair_in, pair_mask, ln_pair_v, w_in_v, ln_tri_v, w_out_v)
    pull_back = jax.vjp(forward, pair_act, ln_pair.astype(jnp.float32), w_in.astype(jnp.float32),
                        ln_tri.astype(jnp.float32), w_out.astype(jnp.float32))[1]
    grad_all = pull_back(grad_out)
    return (grad_all[0], grad_all[1], grad_all[2], grad_all[3], grad_all[4])
```

```python
import functools

import jax
import jax.numpy as jnp
from jax import lax
from jax.experimental import pallas as pl
from jax.experimental.pallas import tpu as pltpu
from jax.sharding import PartitionSpec as P


LN_EPS = 1e-5
F32, BF16 = jnp.float32, jnp.bfloat16
N, ROWS, CH, HALF, TILE, DEV, BIG = 512, 64, 128, 64, 128, 8, 10**10
RB = 16
HR = 32
NCH = 4
STRIDE = 72
PAD = 24
VMEM = 62 * 1024 * 1024


def nn(a, b):
    return lax.dot_general(a, b, (((1,), (0,)), ((), ())), preferred_element_type=F32)


def nt(a, b):
    return lax.dot_general(a, b, (((1,), (1,)), ((), ())), preferred_element_type=F32)


def tn(a, b):
    return lax.dot_general(a, b, (((0,), (0,)), ((), ())), preferred_element_type=F32)


def sigmoid(v):
    return 0.5 * jnp.tanh(0.5 * v) + 0.5


def loop(count, body, unroll=1):
    def step(i, carry):
        body(i)
        return carry

    lax.fori_loop(0, count, step, 0, unroll=unroll)


def call(body, grid, in_specs, out_specs, out_shape, scratch=(), prefetch=0, aliases=None, flops=1000):
    return pl.pallas_call(
        body,
        grid_spec=pltpu.PrefetchScalarGridSpec(num_scalar_prefetch=prefetch, grid=grid, in_specs=in_specs,
                                               out_specs=out_specs, scratch_shapes=list(scratch)),
        out_shape=out_shape,
        input_output_aliases=aliases or {},
        compiler_params=pltpu.CompilerParams(dimension_semantics=("arbitrary",) * len(grid), vmem_limit_bytes=VMEM),
        cost_estimate=pl.CostEstimate(flops=flops, bytes_accessed=flops // 100, transcendentals=0))


def full(shape):
    return pl.BlockSpec(shape, lambda *_: (0,) * len(shape))


def sds(shape, dtype):
    return jax.ShapeDtypeStruct(shape, dtype)


def ln_rows(v, gain, bias):
    mean = jnp.mean(v, axis=-1, keepdims=True)
    cen = v - mean
    var = jnp.mean(cen * cen, axis=-1, keepdims=True)
    return cen * lax.rsqrt(var + LN_EPS) * gain + bias


def ln_kernel(z_ref, g_ref, *rest):
    o_ref, full_ref = rest[-2:]

    def row(r):
        v = ln_rows(z_ref[r], g_ref[0:1], g_ref[1:2]).astype(BF16)
        o_ref[r] = v
        full_ref[r] = v

    loop(RB, row)


def chained(in_specs, args, prev, first_out):
    if prev is None:
        return in_specs, args, {}
    aliases = {len(args) + i: first_out + i for i in range(len(prev))}
    return in_specs + [pl.BlockSpec(memory_space=pl.ANY)] * len(prev), args + list(prev), aliases


def ln_chunk(z, g, t, prev):
    zs = pl.BlockSpec((RB, N, CH), lambda i: (t, 0, 0))
    loc = pl.BlockSpec((RB, N, CH), lambda i: (0, 0, 0))
    in_specs, args, aliases = chained([zs, full((2, CH))], [z, g], prev, 1)
    return call(ln_kernel, (1,), in_specs, [loc, zs], [sds((RB, N, CH), BF16), sds((ROWS, N, CH), BF16)],
                aliases=aliases, flops=BIG)(*args)


def proj_kernel(count, id_ref, *refs):
    z_refs, (m_ref, w_ref) = refs[:count], refs[count:count + 2]
    a_ref, b_ref, sa, sb, buf, sem = refs[-6:]
    step = pl.program_id(0)
    slot = lax.rem(step, 2)

    def copy(j):
        return pltpu.make_async_copy(z_refs[j], buf.at[j % 2], sem.at[j % 2])

    for j in range(count):
        @pl.when(step == j)
        def _():
            if j == 0:
                copy(j).start()
            if j + 1 < count:
                copy(j + 1).start()
            copy(j).wait()

    def row(r):
        base = pl.multiple_of(r * STRIDE, 8)
        for l in range(2):
            p = nt(w_ref[...], buf[slot, r, l * 256:(l + 1) * 256, :])
            m = m_ref[pl.ds(r, 1), l * 256:(l + 1) * 256]
            av = m * sigmoid(p[HALF:TILE]) * p[:HALF]
            bv = m * sigmoid(p[TILE + HALF:]) * p[TILE:TILE + HALF]
            for t in range(2):
                sa[2 * l + t, pl.ds(base, HALF), :] = av[:, t * TILE:(t + 1) * TILE]
                sb[2 * l + t, pl.ds(base, HALF), :] = bv[:, t * TILE:(t + 1) * TILE]

    loop(RB, row)

    def chan(c):
        for l in range(4):
            a_ref[c, :, l * TILE:(l + 1) * TILE] = sa[l, pl.ds(c, RB, stride=STRIDE), :].astype(BF16)
            b_ref[c, :, l * TILE:(l + 1) * TILE] = sb[l, pl.ds(c, RB, stride=STRIDE), :].astype(BF16)

    loop(HALF, chan, 2)


def proj_chunk(ids, first, blocks, mask, w, t, prev):
    count = len(blocks)

    def place(i, s):
        return ((s[0] * 2 + s[1]) ^ (first + i)) * NCH + t

    out = pl.BlockSpec((HALF, RB, N), lambda i, s: (0, place(i, s), 0))
    in_specs, args, aliases = chained(
        [pl.BlockSpec(memory_space=pl.ANY)] * count + [pl.BlockSpec((RB, N), lambda i, s: (place(i, s), 0)),
                                                       full((256, CH))], [*blocks, mask, w], prev, 0)
    return call(functools.partial(proj_kernel, count), (count,), in_specs, [out, out], [sds((HALF, N, N), BF16)] * 2,
                [pltpu.VMEM((4, RB * STRIDE, TILE), F32)] * 2
                + [pltpu.VMEM((2, RB, N, CH), BF16), pltpu.SemaphoreType.DMA((2,))], prefetch=1,
                aliases={k + 1: v for k, v in aliases.items()}, flops=BIG)(ids, *args)


CB = 8


def swap_out(h, v, keep_ref, send_ref, c):
    lo, hi = v[:ROWS].astype(keep_ref.dtype), v[ROWS:].astype(keep_ref.dtype)
    keep_ref[c] = jnp.where(h == 0, lo, hi)
    send_ref[c] = jnp.where(h == 0, hi, lo)


def tri_kernel(form, id_ref, a_ref, b_ref, keep_ref, send_ref):
    h = id_ref[1]

    def chan(c):
        v = nt(a_ref[c], b_ref[c]) if form == 'out' else tn(a_ref[c], b_ref[c])
        lo, hi = v[:ROWS], v[ROWS:]
        keep, send = jnp.where(h == 0, lo, hi), jnp.where(h == 0, hi, lo)
        for l in range(4):
            keep_ref[l, c] = keep[:, l * TILE:(l + 1) * TILE]
            send_ref[l, c] = send[:, l * TILE:(l + 1) * TILE]

    loop(CB, chan)


def tri_forward(form, ids, a, b):
    if form == 'out':
        a_spec = pl.BlockSpec((CB, TILE, N), lambda c, s: (c, s[0], 0))
    else:
        a_spec = pl.BlockSpec((CB, N, TILE), lambda c, s: (c, 0, s[0]))
    half = pl.BlockSpec((4, CB, ROWS, TILE), lambda c, s: (0, c, 0, 0))
    return call(functools.partial(tri_kernel, form), (HALF // CB,),
                [a_spec, pl.BlockSpec((CB, N, N), lambda c, s: (c, 0, 0))], [half, half],
                [sds((4, HALF, ROWS, TILE), F32)] * 2, prefetch=1, flops=BIG)(ids, a, b)


def row_ds(start, size):
    return pl.ds(pl.multiple_of(start, size), size)


def fill_dx(h, halves, c, dx):
    for e in range(2):
        for o in range(2):
            dx[row_ds((h ^ o) * ROWS + e * HR, HR), :] = halves[2 * e + o][c]


def da_out_kernel(id_ref, b_ref, *rest):
    halves, (keep_ref, send_ref, dx) = rest[:4], rest[-3:]
    h = id_ref[1]

    def chan(c):
        fill_dx(h, halves, c, dx)
        swap_out(h, nn(dx[...], b_ref[c]), keep_ref, send_ref, c)

    loop(CB, chan)


def da_in_kernel(id_ref, b_ref, *rest):
    halves, outs, (dx, res) = rest[:4], rest[-10:-2], rest[-2:]
    idx = id_ref[0] * 2 + id_ref[1]

    def chan(c):
        fill_dx(id_ref[1], halves, c, dx)
        res[...] = nt(b_ref[c].reshape(DEV * HR, N), dx[...]).astype(BF16)
        for s in range(DEV):
            outs[s][c] = res[row_ds((idx ^ s) * HR, HR), :]

    loop(CB, chan)


def fill_pieces(idx, pieces, c, dx):
    for e in range(2):
        for s in range(DEV):
            dx[row_ds((idx ^ s) * ROWS + e * HR, HR), :] = pieces[e * DEV + s][c]


def db_out_kernel(id_ref, a_ref, *rest):
    pieces, (keep_ref, send_ref, dx) = rest[:2 * DEV], rest[-3:]

    def chan(c):
        fill_pieces(id_ref[0] * 2 + id_ref[1], pieces, c, dx)
        swap_out(id_ref[1], tn(dx[...], a_ref[c]), keep_ref, send_ref, c)

    loop(CB, chan)


def db_in_kernel(id_ref, a_ref, *rest):
    pieces, outs, (dx, res) = rest[:2 * DEV], rest[-10:-2], rest[-2:]
    idx = id_ref[0] * 2 + id_ref[1]

    def chan(c):
        fill_pieces(idx, pieces, c, dx)
        res[...] = nn(a_ref[c].reshape(DEV * HR, N), dx[...]).astype(BF16)
        for s in range(DEV):
            outs[s][c] = res[row_ds((idx ^ s) * HR, HR), :]

    loop(CB, chan)


def tri_back(kind, ids, mat, parts, half=None, after=()):
    rows = pl.BlockSpec((CB, HR, parts[0].shape[2]), lambda c, s: (c, 0, 0))
    dx = pltpu.VMEM((TILE, N) if kind.startswith('da') else (N, TILE), BF16)
    tail = [pl.BlockSpec(memory_space=pl.ANY)] * len(after)
    bodies = {'da_out': da_out_kernel, 'db_out': db_out_kernel, 'da_in': da_in_kernel, 'db_in': db_in_kernel}
    if half is None:
        keep = pl.BlockSpec((CB, ROWS, N), lambda c, s: (c, 0, 0))
        return call(bodies[kind], (HALF // CB,),
                    [pl.BlockSpec((CB, N, N), lambda c, s: (c, 0, 0))] + [rows] * len(parts) + tail, [keep, keep],
                    [sds((HALF, ROWS, N), BF16)] * 2, [dx], prefetch=1, flops=BIG)(ids, mat, *parts, *after)
    piece = pl.BlockSpec((CB, HR, TILE), lambda c, s: (c, 0, 0))
    return call(bodies[kind], (HALF // CB,),
                [pl.BlockSpec((CB, DEV, HR, N), lambda c, s: (c, 0, half, 0))] + [rows] * len(parts) + tail,
                [piece] * DEV, [sds((HALF, HR, TILE), BF16)] * DEV, [dx, pltpu.VMEM((DEV * HR, TILE), BF16)],
                prefetch=1, flops=BIG)(ids, mat.reshape(HALF, DEV, ROWS, N), *parts, *after)


def x_row(xk_ref, xr_ref, r, rb):
    halves = []
    for ref in (xk_ref, xr_ref):
        flat = ref.reshape(4, HALF * rb, TILE)
        halves.append(jnp.concatenate([flat[l, pl.ds(r, HALF, stride=rb), :] for l in range(4)], axis=1))
    return jnp.concatenate(halves, axis=0)


def x_norm(x):
    mean = jnp.mean(x, axis=0, keepdims=True)
    cen = x - mean
    rstd = lax.rsqrt(jnp.mean(cen * cen, axis=0, keepdims=True) + LN_EPS)
    return cen * rstd, rstd


def fin_kernel(xk_ref, xr_ref, z_ref, zn_ref, wg_ref, wo_ref, gt_ref, g1_ref, *rest):
    loc_ref, z1_ref, zn1_ref = rest[-3:]

    def row(r):
        xhat, _ = x_norm(x_row(xk_ref, xr_ref, r, RB))
        xn = (xhat * gt_ref[:, 0:1] + gt_ref[:, 1:2]).astype(BF16)
        gate = sigmoid(nn(zn_ref[r], wg_ref[...]))
        z1 = z_ref[r] + gate * tn(xn, wo_ref[...])
        z1_ref[r] = z1
        zn1 = ln_rows(z1, g1_ref[0:1], g1_ref[1:2]).astype(BF16)
        loc_ref[r] = zn1
        zn1_ref[r] = zn1

    loop(RB, row)


def fin_chunk(xk, xr, z, zn, wg, wo, gt, g1, t, prev):
    xs = pl.BlockSpec((4, HALF, RB, TILE), lambda i: (0, 0, t, 0))
    zs = pl.BlockSpec((RB, N, CH), lambda i: (t, 0, 0))
    loc = pl.BlockSpec((RB, N, CH), lambda i: (0, 0, 0))
    in_specs, args, aliases = chained([xs, xs, zs, zs, full((CH, CH)), full((CH, CH)), full((CH, 2)), full((2, CH))],
                                      [xk, xr, z, zn, wg, wo, gt, g1], prev, 1)
    return call(fin_kernel, (1,), in_specs, [loc, zs, zs],
                [sds((RB, N, CH), BF16), sds((ROWS, N, CH), F32), sds((ROWS, N, CH), BF16)],
                aliases=aliases, flops=BIG)(*args)


def finb_kernel(id_ref, xk_ref, xr_ref, zn_ref, dz_ref, wg_ref, wo_ref, gt_ref, *rest):
    dg_ref, dk_ref, ds_ref = rest[-15:-12]
    pieces, (dwo_ref, dga_ref, dbi_ref, sd) = rest[-12:-4], rest[-4:]

    @pl.when(pl.program_id(0) == 0)
    def _():
        dwo_ref[...] = jnp.zeros_like(dwo_ref)
        dga_ref[...] = jnp.zeros_like(dga_ref)
        dbi_ref[...] = jnp.zeros_like(dbi_ref)

    def row(r):
        base = pl.multiple_of(r * STRIDE, 8)
        xhat, rstd = x_norm(x_row(xk_ref, xr_ref, r, RB))
        gain = gt_ref[:, 0:1]
        xn = (xhat * gain + gt_ref[:, 1:2]).astype(BF16)
        gate = sigmoid(nn(zn_ref[r], wg_ref[...]))
        proj = tn(xn, wo_ref[...])
        dz = dz_ref[r]
        gated = dz * gate
        dg_ref[r] = (gated * proj * (1.0 - gate)).astype(BF16)
        dproj = gated.astype(BF16)
        dwo_ref[...] += nn(xn, dproj)
        dn = nt(wo_ref[...], dproj).astype(BF16).astype(F32)
        prod = dn * xhat
        dga, dbi = dga_ref[...], dbi_ref[...]
        for l in range(4):
            dga += prod[:, l * TILE:(l + 1) * TILE]
            dbi += dn[:, l * TILE:(l + 1) * TILE]
        dga_ref[...] = dga
        dbi_ref[...] = dbi
        dxh = dn * gain
        m1 = jnp.mean(dxh, axis=0, keepdims=True)
        m2 = jnp.mean(dxh * xhat, axis=0, keepdims=True)
        dx = rstd * (dxh - m1 - xhat * m2)
        for e in range(2):
            for l in range(4):
                sd[e, l, pl.ds(base, HALF), :] = dx[e * HALF:(e + 1) * HALF, l * TILE:(l + 1) * TILE]

    loop(RB, row, 2)
    q = id_ref[0]

    def chan(c):
        for l in range(4):
            dk_ref[c, :, l * TILE:(l + 1) * TILE] = sd[0, l, pl.ds(c, RB, stride=STRIDE), :].astype(BF16)
            ds_ref[c, :, l * TILE:(l + 1) * TILE] = sd[1, l, pl.ds(c, RB, stride=STRIDE), :].astype(BF16)
        for s in range(DEV):
            pieces[s][c] = sd[s & 1, q ^ (s >> 1), pl.ds(c, RB, stride=STRIDE), :].astype(BF16)

    loop(HALF, chan, 2)


def part_spec(v, e):
    off = e * (HR // RB) if v.shape[0] == ROWS else 0
    return pl.BlockSpec((RB,) + v.shape[1:], lambda i, s: (off + i,) + (0,) * (v.ndim - 1))


def fin_back(e, ids, xk, xr, zn, dz, wg, wo, gt, after=()):
    x4 = pl.BlockSpec((4, HALF, RB, TILE), lambda i, s: (0, 0, e * (HR // RB) + i, 0))
    xs = pl.BlockSpec((HALF, RB, N), lambda i, s: (0, i, 0))
    ps = pl.BlockSpec((HALF, RB, TILE), lambda i, s: (0, i, 0))
    dgs = pl.BlockSpec((RB, N, CH), lambda i, s: (i, 0, 0))
    acc = full((CH, CH))
    return call(finb_kernel, (HR // RB,), [x4, x4, part_spec(zn, e), part_spec(dz, e), acc, acc, full((CH, 2))]
                + [pl.BlockSpec(memory_space=pl.ANY)] * len(after),
                [dgs, xs, xs] + [ps] * DEV + [acc] * 3,
                [sds((HR, N, CH), BF16)] + [sds((HALF, HR, N), BF16)] * 2 + [sds((HALF, HR, TILE), BF16)] * DEV
                + [sds((CH, CH), F32)] * 3,
                [pltpu.VMEM((2, 4, RB * STRIDE, TILE), F32)], prefetch=1, flops=BIG)(
                    ids, xk, xr, zn, dz, wg, wo, gt, *after)


def projb_kernel(form, id_ref, *refs):
    n = 2 if form == 'out' else 8
    da, db = refs[:n], refs[n:2 * n]
    zn_ref, z_ref, dz_ref, dg_ref, m_ref, w_ref, wg_ref, g_ref = refs[2 * n:2 * n + DEV]
    o_ref, dw_ref, dwg_ref, dga_ref, dbi_ref, sa, sb = refs[-7:]
    q = id_ref[0]

    @pl.when(pl.program_id(0) == 0)
    def _():
        for ref in (dw_ref, dwg_ref, dga_ref, dbi_ref):
            ref[...] = jnp.zeros_like(ref)

    def chan(c):
        base = pl.multiple_of(c * PAD, 8)
        for src, dst in ((da, sa), (db, sb)):
            for s in range(n):
                if form == 'out':
                    for l in range(4):
                        dst[s, l, pl.ds(base, RB), :] = src[s][c, :, l * TILE:(l + 1) * TILE].astype(F32)
                else:
                    dst[s & 1, q ^ (s >> 1), pl.ds(base, RB), :] = src[s][c].astype(F32)

    loop(HALF, chan, 2)

    def row(r):
        zn = zn_ref[r]
        m = m_ref[pl.ds(r, 1), :]
        dg = dg_ref[r]
        dzn = nt(dg, wg_ref[...])
        dwg_ref[...] += tn(zn, dg)
        for e in range(2):
            w = w_ref[e * 256:(e + 1) * 256, :]
            p = nt(w, zn)
            parts = []
            for k, src in enumerate((sa, sb)):
                d = jnp.concatenate([src[e, l, pl.ds(r, HALF, stride=PAD), :] for l in range(4)], axis=1) * m
                lin = p[k * TILE:k * TILE + 64]
                sig = sigmoid(p[k * TILE + 64:k * TILE + TILE])
                ds = d * sig
                parts += [ds.astype(BF16), (ds * lin * (1.0 - sig)).astype(BF16)]
            cat = jnp.concatenate(parts, axis=0)
            dzn += tn(cat, w)
            dw_ref[e * 256:(e + 1) * 256, :] += nn(cat, zn)
        dn = dzn.astype(BF16).astype(F32)
        z = z_ref[r]
        mean = jnp.mean(z, axis=-1, keepdims=True)
        cen = z - mean
        rstd = lax.rsqrt(jnp.mean(cen * cen, axis=-1, keepdims=True) + LN_EPS)
        zhat = cen * rstd
        dga_ref[...] += jnp.sum((dn * zhat).reshape(N // 8, 8, CH), axis=0)
        dbi_ref[...] += jnp.sum(dn.reshape(N // 8, 8, CH), axis=0)
        dh = dn * g_ref[0:1]
        m1 = jnp.mean(dh, axis=-1, keepdims=True)
        m2 = jnp.mean(dh * zhat, axis=-1, keepdims=True)
        o_ref[r] = dz_ref[r] + rstd * (dh - m1 - zhat * m2)

    loop(RB, row, 2)


def proj_back(form, e, ids, da, db, zn, z, dz, dg, mask, w, wg, g, prev=None, after=()):
    off = e * (HR // RB)
    if form == 'out':
        ps = pl.BlockSpec((HALF, RB, N), lambda i, s: (0, off + i, 0))
        o_spec, o_rows = part_spec(z, e), ROWS
    else:
        ps = pl.BlockSpec((HALF, RB, TILE), lambda i, s: (0, i, 0))
        o_spec, o_rows = pl.BlockSpec((RB, N, CH), lambda i, s: (i, 0, 0)), HR
    rows = [zn, z, dz, dg, mask]
    in_specs, args, aliases = chained(
        [ps] * (2 * len(da)) + [part_spec(v, e) for v in rows] + [full((512, CH)), full((CH, CH)), full((2, CH))],
        [*da, *db, *rows, w, wg, g], prev, 0)
    return call(functools.partial(projb_kernel, form), (HR // RB,),
                in_specs + [pl.BlockSpec(memory_space=pl.ANY)] * len(after),
                [o_spec, full((512, CH)), full((CH, CH)), full((DEV, CH)), full((DEV, CH))],
                [sds((o_rows, N, CH), F32), sds((512, CH), F32), sds((CH, CH), F32), sds((DEV, CH), F32),
                 sds((DEV, CH), F32)],
                [pltpu.VMEM((2, 4, HALF * PAD, TILE), F32)] * 2, prefetch=1,
                aliases={k + 1: v for k, v in aliases.items()}, flops=2 * BIG)(
                    ids, *args, *after)


def solution(mesh):
    row_spec = P(('data', 'dap'))
    grad_spec = P('data')

    def xor(v, s):
        if s == 0:
            return v
        return lax.ppermute(v, 'dap', [(i, i ^ s) for i in range(DEV)])

    def device_body(pair_act, pair_mask, grad_out, ln_pair, w_in, ln_tri, w_out):
        idx = lax.axis_index('dap').astype(jnp.int32)
        h = lax.rem(idx, 2)
        ids = jnp.stack([idx // 2, h])
        mask = pair_mask.astype(F32)
        mask_all = lax.all_gather(mask, 'dap', axis=0, tiled=True)
        g_pair = ln_pair.astype(F32)
        g_tri = ln_tri.astype(F32)

        def rel(v, axis):
            lo, hi = jnp.split(v, 2, axis=axis)
            return jnp.where(h == 0, v, jnp.concatenate([hi, lo], axis=axis))

        w_rel, wg, wo_rel, gt_rel = [], [], [], []
        for u in range(2):
            wt = w_in[u, :, :512].T.reshape(4, 2, HALF, CH).transpose(1, 0, 2, 3).reshape(512, CH)
            w_rel.append(rel(wt, 0))
            wg.append(w_in[u, :, 512:])
            wo_rel.append(rel(w_out[u], 0))
            gt_rel.append(rel(g_tri[u].T, 0))

        def spread(v):
            return [v] + [xor(v, s) for s in (1, 2, 4)]

        def gather_proj(parts, u):
            w, prev = w_rel[u][:256], None
            for t, (own, r1, _, _) in enumerate(parts):
                prev = proj_chunk(ids, 0, [own, r1], mask_all, w, t, prev)
            far = []
            for t, (_, _, r2, r4) in enumerate(parts):
                far.append(xor(r4, 2) if t % 2 else xor(r2, 4))
                near = [r2, xor(r2, 1), r4, xor(r4, 1)]
                prev = proj_chunk(ids, 2, near, mask_all, w, t, prev)
            for t, r6 in enumerate(far):
                r7 = xor(r6, 1)
                prev = proj_chunk(ids, 6, [r6, r7], mask_all, w, t, prev)
            return prev

        parts, prev = [], None
        for t in range(NCH):
            chunk, zn0 = ln_chunk(pair_act, g_pair[0], t, prev)
            parts, prev = parts + [spread(chunk)], [zn0]
        a0, b0 = gather_proj(parts, 0)
        x0k, x0s = tri_forward('out', ids, a0, b0)
        x0r = xor(x0s, 1)
        parts, prev = [], None
        for t in range(NCH):
            chunk, z1, zn1 = fin_chunk(x0k, x0r, pair_act, zn0, wg[0], wo_rel[0], gt_rel[0], g_pair[1], t, prev)
            parts, prev = parts + [spread(chunk)], [z1, zn1]
        a1, b1 = gather_proj(parts, 1)
        x1k, x1s = tri_forward('in', ids, a1, b1)
        x1r = xor(x1s, 1)

        def exchange(pieces):
            return [xor(v, s) for s, v in enumerate(pieces)]

        def split(out):
            dg, dk, ds = out[:3]
            return dg, [dk, xor(ds, 1)], exchange(out[3:11]), out[11:], dk

        fb1 = [split(fin_back(0, ids, x1k, x1r, zn1, grad_out, wg[1], wo_rel[1], gt_rel[1]))]
        out = fin_back(1, ids, x1k, x1r, zn1, grad_out, wg[1], wo_rel[1], gt_rel[1], (fb1[0][4],))
        fb1 += [split(out)]
        dx1, dp1 = fb1[0][1] + fb1[1][1], fb1[0][2] + fb1[1][2]
        da, db, last = [], [], fb1[1][4]
        for e in range(2):
            out = tri_back('da_in', ids, b1, dx1, e, (last,))
            da.append(exchange(out))
            out = tri_back('db_in', ids, a1, dp1, e, (out[0],))
            db.append(exchange(out))
            last = out[0]
        pb1, fb0 = [], []
        for e in range(2):
            pb1.append(proj_back('in', e, ids, da[e], db[e], zn1, z1, grad_out, fb1[e][0], mask, w_rel[1], wg[1],
                                 g_pair[1], after=(last,)))
            fb0.append(split(fin_back(e, ids, x0k, x0r, zn0, pb1[e][0], wg[0], wo_rel[0], gt_rel[0])))
            last = fb0[e][4]
        da_k, da_s = tri_back('da_out', ids, b0, fb0[0][1] + fb0[1][1])
        da_0 = [da_k, xor(da_s, 1)]
        db_k, db_s = tri_back('db_out', ids, a0, fb0[0][2] + fb0[1][2], after=(da_k,))
        db_0 = [db_k, xor(db_s, 1)]
        pb0, prev = [], None
        for e in range(2):
            pb0.append(proj_back('out', e, ids, da_0, db_0, zn0, pair_act, pb1[e][0], fb0[e][0], mask, w_rel[0], wg[0],
                                 g_pair[0], prev=prev))
            prev = [pb0[e][0]]

        def pack(fb, pb):
            dwo, dga, dbi = [fb[0][3][i] + fb[1][3][i] for i in range(3)]
            dw, dwg, dgp, dbp = [pb[0][i] + pb[1][i] for i in range(1, 5)]
            dw = rel(dw, 0).reshape(2, 4, HALF, CH).transpose(1, 0, 2, 3).reshape(512, CH)
            tri = jnp.stack([jnp.sum(rel(dga, 0), 1), jnp.sum(rel(dbi, 0), 1)])
            return lax.psum(jnp.concatenate([dw, dwg, rel(dwo, 0), dgp, dbp, tri], axis=0), 'dap')

        def unpack(v):
            dw, dwg, dwo, dgp, dbp, tri = jnp.split(v, [512, 640, 768, 776, 784])
            return (jnp.stack([jnp.sum(dgp, 0), jnp.sum(dbp, 0)]), jnp.concatenate([dw.T, dwg], axis=1), tri, dwo)

        packed = [pack(fb0, pb0), pack(fb1, pb1)]
        return (pb0[1][0],) + tuple(jnp.stack(v) for v in zip(*[unpack(v) for v in packed]))


    return jax.shard_map(device_body, mesh=mesh,
                         in_specs=(row_spec, row_spec, row_spec, P(), P(), P(), P()),
                         out_specs=(row_spec, grad_spec, grad_spec, grad_spec, grad_spec),
                         check_vma=False)
```

```python
import functools

import jax
import jax.numpy as jnp
from jax import lax
from jax.experimental import pallas as pl
from jax.experimental.pallas import tpu as pltpu
from jax.sharding import PartitionSpec as P


LN_EPS = 1e-5
F32, BF16 = jnp.float32, jnp.bfloat16
N, ROWS, CH, HALF, TILE, DEV, BIG = 512, 64, 128, 64, 128, 8, 10**10
RB = 16
HR = 32
NCH = 4
STRIDE = 72
PAD = 24
HOPS = (1, 2, 4)
VMEM = 62 * 1024 * 1024


def nn(a, b):
    return lax.dot_general(a, b, (((1,), (0,)), ((), ())), preferred_element_type=F32)


def nt(a, b):
    return lax.dot_general(a, b, (((1,), HOPS[:1]), ((), ())), preferred_element_type=F32)


def tn(a, b):
    return lax.dot_general(a, b, (((0,), (0,)), ((), ())), preferred_element_type=F32)


def sigmoid(v):
    return 0.5 * jnp.tanh(0.5 * v) + 0.5


def loop(count, body, unroll=1):
    def step(i, carry):
        body(i)
        return carry

    lax.fori_loop(0, count, step, 0, unroll=unroll)


def call(body, grid, in_specs, out_specs, out_shape, scratch=(), prefetch=0, aliases=None, flops=1000):
    return pl.pallas_call(
        body,
        grid_spec=pltpu.PrefetchScalarGridSpec(num_scalar_prefetch=prefetch, grid=grid, in_specs=in_specs,
                                               out_specs=out_specs, scratch_shapes=list(scratch)),
        out_shape=out_shape,
        input_output_aliases=aliases or {},
        compiler_params=pltpu.CompilerParams(dimension_semantics=("arbitrary",) * len(grid), vmem_limit_bytes=VMEM),
        cost_estimate=pl.CostEstimate(flops=flops, bytes_accessed=flops // 100, transcendentals=0))


def full(shape):
    return pl.BlockSpec(shape, lambda *_: (0,) * len(shape))


def sds(shape, dtype):
    return jax.ShapeDtypeStruct(shape, dtype)


def ln_rows(v, gain, bias):
    mean = jnp.mean(v, axis=-1, keepdims=True)
    cen = v - mean
    var = jnp.mean(cen * cen, axis=-1, keepdims=True)
    return cen * lax.rsqrt(var + LN_EPS) * gain + bias


def ln_kernel(z_ref, g_ref, *rest):
    o_ref, full_ref = rest[-2:]

    def row(r):
        v = ln_rows(z_ref[r], g_ref[0:1], g_ref[1:2]).astype(BF16)
        o_ref[r] = v
        full_ref[r] = v

    loop(RB, row)


def chained(in_specs, args, prev, first_out):
    if prev is None:
        return in_specs, args, {}
    aliases = {len(args) + i: first_out + i for i in range(len(prev))}
    return in_specs + [pl.BlockSpec(memory_space=pl.ANY)] * len(prev), args + list(prev), aliases


def ln_chunk(z, g, t, prev):
    zs = pl.BlockSpec((RB, N, CH), lambda i: (t, 0, 0))
    loc = pl.BlockSpec((RB, N, CH), lambda i: (0, 0, 0))
    in_specs, args, aliases = chained([zs, full((2, CH))], [z, g], prev, 1)
    return call(ln_kernel, (1,), in_specs, [loc, zs], [sds((RB, N, CH), BF16), sds((ROWS, N, CH), BF16)],
                aliases=aliases, flops=BIG)(*args)


def proj_kernel(count, id_ref, *refs):
    z_refs, m_refs, w_ref = refs[:count], refs[count:2 * count], refs[2 * count]
    a_ref, b_ref, sa, sb, buf, m_ref, sem = refs[-7:]
    step = pl.program_id(0)
    slot = lax.rem(step, 2)

    def copy(j):
        return pltpu.make_async_copy(z_refs[j], buf.at[j % 2], sem.at[j % 2])

    for j in range(count):
        @pl.when(step == j)
        def _():
            if j == 0:
                copy(j).start()
            if j + 1 < count:
                copy(j + 1).start()
            m_ref[...] = m_refs[j][...]
            copy(j).wait()

    def row(r):
        base = pl.multiple_of(r * STRIDE, 8)
        for l in range(2):
            p = nt(w_ref[...], buf[slot, r, l * 256:(l + 1) * 256, :])
            m = m_ref[pl.ds(r, 1), l * 256:(l + 1) * 256]
            av = m * sigmoid(p[HALF:TILE]) * p[:HALF]
            bv = m * sigmoid(p[TILE + HALF:]) * p[TILE:TILE + HALF]
            for t in range(2):
                sa[2 * l + t, pl.ds(base, HALF), :] = av[:, t * TILE:(t + 1) * TILE]
                sb[2 * l + t, pl.ds(base, HALF), :] = bv[:, t * TILE:(t + 1) * TILE]

    loop(RB, row)

    def chan(c):
        for l in range(4):
            a_ref[c, :, l * TILE:(l + 1) * TILE] = sa[l, pl.ds(c, RB, stride=STRIDE), :].astype(BF16)
            b_ref[c, :, l * TILE:(l + 1) * TILE] = sb[l, pl.ds(c, RB, stride=STRIDE), :].astype(BF16)

    loop(HALF, chan, 2)


def proj_chunk(ids, first, width, blocks, masks, w, t, prev):
    count = len(blocks)

    def place(i, s):
        return ((s[0] * 2 + s[1]) ^ (first + lax.rem(i, width))) * NCH + t + lax.div(i, width)

    def mask_spec(j):
        return pl.BlockSpec((RB, N), lambda i, s: (t + j // width, 0))

    out = pl.BlockSpec((HALF, RB, N), lambda i, s: (0, place(i, s), 0))
    in_specs, args, aliases = chained(
        [pl.BlockSpec(memory_space=pl.ANY)] * count + [mask_spec(j) for j in range(count)] + [full((256, CH))],
        [*blocks, *[masks[first + j % width] for j in range(count)], w], prev, 0)
    return call(functools.partial(proj_kernel, count), (count,), in_specs, [out, out], [sds((HALF, N, N), BF16)] * 2,
                [pltpu.VMEM((4, RB * STRIDE, TILE), F32)] * 2
                + [pltpu.VMEM((2, RB, N, CH), BF16), pltpu.VMEM((RB, N), F32), pltpu.SemaphoreType.DMA((2,))],
                prefetch=1, aliases={k + 1: v for k, v in aliases.items()}, flops=BIG)(ids, *args)


CB = 8


def swap_out(h, v, keep_ref, send_ref, c):
    lo, hi = v[:ROWS].astype(keep_ref.dtype), v[ROWS:].astype(keep_ref.dtype)
    keep_ref[c] = jnp.where(h == 0, lo, hi)
    send_ref[c] = jnp.where(h == 0, hi, lo)


def tri_kernel(form, id_ref, a_ref, b_ref, *rest):
    keep_ref, send_ref = rest[-2:]
    h = id_ref[1]

    def chan(c):
        v = nt(a_ref[c], b_ref[c]) if form == 'out' else tn(a_ref[c], b_ref[c])
        lo, hi = v[:ROWS], v[ROWS:]
        keep, send = jnp.where(h == 0, lo, hi), jnp.where(h == 0, hi, lo)
        for l in range(4):
            keep_ref[l, c] = keep[:, l * TILE:(l + 1) * TILE]
            send_ref[l, c] = send[:, l * TILE:(l + 1) * TILE]

    loop(CB, chan)


def tri_forward(form, part, ids, a, b, after=()):
    off = part * (HR // CB)
    if form == 'out':
        a_spec = pl.BlockSpec((CB, TILE, N), lambda c, s: (off + c, s[0], 0))
    else:
        a_spec = pl.BlockSpec((CB, N, TILE), lambda c, s: (off + c, 0, s[0]))
    half = pl.BlockSpec((4, CB, ROWS, TILE), lambda c, s: (0, c, 0, 0))
    return call(functools.partial(tri_kernel, form), (HR // CB,),
                [a_spec, pl.BlockSpec((CB, N, N), lambda c, s: (off + c, 0, 0))]
                + [pl.BlockSpec(memory_space=pl.ANY)] * len(after), [half, half],
                [sds((4, HR, ROWS, TILE), F32)] * 2, prefetch=1, flops=BIG)(ids, a, b, *after)


def row_ds(start, size):
    return pl.ds(pl.multiple_of(start, size), size)


def fill_dx(h, halves, c, dx):
    for e in range(2):
        for o in range(2):
            dx[row_ds((h ^ o) * ROWS + e * HR, HR), :] = halves[2 * e + o][c]


def da_out_kernel(id_ref, b_ref, *rest):
    halves, (keep_ref, send_ref, dx) = rest[:4], rest[-3:]
    h = id_ref[1]

    def chan(c):
        fill_dx(h, halves, c, dx)
        swap_out(h, nn(dx[...], b_ref[c]), keep_ref, send_ref, c)

    loop(CB, chan)


def da_in_kernel(id_ref, b_ref, *rest):
    halves, outs, (dx, res) = rest[:4], rest[-10:-2], rest[-2:]
    idx = id_ref[0] * 2 + id_ref[1]

    def chan(c):
        fill_dx(id_ref[1], halves, c, dx)
        res[...] = nt(b_ref[c].reshape(DEV * HR, N), dx[...]).astype(BF16)
        for s in range(DEV):
            outs[s][c] = res[row_ds((idx ^ s) * HR, HR), :]

    loop(CB, chan)


def fill_pieces(idx, pieces, c, dx):
    for e in range(2):
        for s in range(DEV):
            dx[row_ds((idx ^ s) * ROWS + e * HR, HR), :] = pieces[e * DEV + s][c]


def db_out_kernel(id_ref, a_ref, *rest):
    pieces, (keep_ref, send_ref, dx) = rest[:2 * DEV], rest[-3:]

    def chan(c):
        fill_pieces(id_ref[0] * 2 + id_ref[1], pieces, c, dx)
        swap_out(id_ref[1], tn(dx[...], a_ref[c]), keep_ref, send_ref, c)

    loop(CB, chan)


def db_in_kernel(id_ref, a_ref, *rest):
    pieces, outs, (dx, res) = rest[:2 * DEV], rest[-10:-2], rest[-2:]
    idx = id_ref[0] * 2 + id_ref[1]

    def chan(c):
        fill_pieces(idx, pieces, c, dx)
        res[...] = nn(a_ref[c].reshape(DEV * HR, N), dx[...]).astype(BF16)
        for s in range(DEV):
            outs[s][c] = res[row_ds((idx ^ s) * HR, HR), :]

    loop(CB, chan)


def tri_back(kind, ids, mat, parts, half=None, after=()):
    rows = pl.BlockSpec((CB, HR, parts[0].shape[2]), lambda c, s: (c, 0, 0))
    dx = pltpu.VMEM((TILE, N) if kind.startswith('da') else (N, TILE), BF16)
    tail = [pl.BlockSpec(memory_space=pl.ANY)] * len(after)
    bodies = {'da_out': da_out_kernel, 'db_out': db_out_kernel, 'da_in': da_in_kernel, 'db_in': db_in_kernel}
    if half is None:
        keep = pl.BlockSpec((CB, ROWS, N), lambda c, s: (c, 0, 0))
        return call(bodies[kind], (HALF // CB,),
                    [pl.BlockSpec((CB, N, N), lambda c, s: (c, 0, 0))] + [rows] * len(parts) + tail, [keep, keep],
                    [sds((HALF, ROWS, N), BF16)] * 2, [dx], prefetch=1, flops=BIG)(ids, mat, *parts, *after)
    piece = pl.BlockSpec((CB, HR, TILE), lambda c, s: (c, 0, 0))
    return call(bodies[kind], (HALF // CB,),
                [pl.BlockSpec((CB, DEV, HR, N), lambda c, s: (c, 0, half, 0))] + [rows] * len(parts) + tail,
                [piece] * DEV, [sds((HALF, HR, TILE), BF16)] * DEV, [dx, pltpu.VMEM((DEV * HR, TILE), BF16)],
                prefetch=1, flops=BIG)(ids, mat.reshape(HALF, DEV, ROWS, N), *parts, *after)


def x_row(x_refs, r):
    parts = []
    for ref in x_refs:
        flat = ref.reshape(4, HR * RB, TILE)
        parts.append(jnp.concatenate([flat[l, pl.ds(r, HR, stride=RB), :] for l in range(4)], axis=1))
    return jnp.concatenate(parts, axis=0)


def x_norm(x):
    mean = jnp.mean(x, axis=0, keepdims=True)
    cen = x - mean
    rstd = lax.rsqrt(jnp.mean(cen * cen, axis=0, keepdims=True) + LN_EPS)
    return cen * rstd, rstd


def fin_kernel(*refs):
    x_refs, (z_ref, zn_ref, wg_ref, wo_ref, gt_ref, g1_ref, *rest) = refs[:4], refs[4:]
    loc_ref, z1_ref, zn1_ref = rest[-3:]

    def row(r):
        xhat, _ = x_norm(x_row(x_refs, r))
        xn = (xhat * gt_ref[:, 0:1] + gt_ref[:, 1:2]).astype(BF16)
        gate = sigmoid(nn(zn_ref[r], wg_ref[...]))
        z1 = z_ref[r] + gate * tn(xn, wo_ref[...])
        z1_ref[r] = z1
        zn1 = ln_rows(z1, g1_ref[0:1], g1_ref[1:2]).astype(BF16)
        loc_ref[r] = zn1
        zn1_ref[r] = zn1

    loop(RB, row)


def fin_chunk(x, z, zn, wg, wo, gt, g1, t, prev):
    xs = pl.BlockSpec((4, HR, RB, TILE), lambda i: (0, 0, t, 0))
    zs = pl.BlockSpec((RB, N, CH), lambda i: (t, 0, 0))
    loc = pl.BlockSpec((RB, N, CH), lambda i: (0, 0, 0))
    in_specs, args, aliases = chained([xs] * 4 + [zs, zs, full((CH, CH)), full((CH, CH)), full((CH, 2)), full((2, CH))],
                                      [*x, z, zn, wg, wo, gt, g1], prev, 1)
    return call(fin_kernel, (1,), in_specs, [loc, zs, zs],
                [sds((RB, N, CH), BF16), sds((ROWS, N, CH), F32), sds((ROWS, N, CH), BF16)],
                aliases=aliases, flops=BIG)(*args)


def finb_kernel(id_ref, *refs):
    x_refs, (zn_ref, dz_ref, wg_ref, wo_ref, gt_ref, *rest) = refs[:4], refs[4:]
    dg_ref, dk_ref, ds_ref = rest[-15:-12]
    pieces, (dwo_ref, dga_ref, dbi_ref, sd) = rest[-12:-4], rest[-4:]

    @pl.when(pl.program_id(0) == 0)
    def _():
        dwo_ref[...] = jnp.zeros_like(dwo_ref)
        dga_ref[...] = jnp.zeros_like(dga_ref)
        dbi_ref[...] = jnp.zeros_like(dbi_ref)

    def row(r):
        base = pl.multiple_of(r * STRIDE, 8)
        xhat, rstd = x_norm(x_row(x_refs, r))
        gain = gt_ref[:, 0:1]
        xn = (xhat * gain + gt_ref[:, 1:2]).astype(BF16)
        gate = sigmoid(nn(zn_ref[r], wg_ref[...]))
        proj = tn(xn, wo_ref[...])
        dz = dz_ref[r]
        gated = dz * gate
        dg_ref[r] = (gated * proj * (1.0 - gate)).astype(BF16)
        dproj = gated.astype(BF16)
        dwo_ref[...] += nn(xn, dproj)
        dn = nt(wo_ref[...], dproj).astype(BF16).astype(F32)
        prod = dn * xhat
        dga, dbi = dga_ref[...], dbi_ref[...]
        for l in range(4):
            dga += prod[:, l * TILE:(l + 1) * TILE]
            dbi += dn[:, l * TILE:(l + 1) * TILE]
        dga_ref[...] = dga
        dbi_ref[...] = dbi
        dxh = dn * gain
        m1 = jnp.mean(dxh, axis=0, keepdims=True)
        m2 = jnp.mean(dxh * xhat, axis=0, keepdims=True)
        dx = rstd * (dxh - m1 - xhat * m2)
        for e in range(2):
            for l in range(4):
                sd[e, l, pl.ds(base, HALF), :] = dx[e * HALF:(e + 1) * HALF, l * TILE:(l + 1) * TILE]

    loop(RB, row, 2)
    q = id_ref[0]

    def chan(c):
        for l in range(4):
            dk_ref[c, :, l * TILE:(l + 1) * TILE] = sd[0, l, pl.ds(c, RB, stride=STRIDE), :].astype(BF16)
            ds_ref[c, :, l * TILE:(l + 1) * TILE] = sd[1, l, pl.ds(c, RB, stride=STRIDE), :].astype(BF16)
        for s in range(DEV):
            pieces[s][c] = sd[s & 1, q ^ (s >> 1), pl.ds(c, RB, stride=STRIDE), :].astype(BF16)

    loop(HALF, chan, 2)


def part_spec(v, e):
    off = e * (HR // RB) if v.shape[0] == ROWS else 0
    return pl.BlockSpec((RB,) + v.shape[1:], lambda i, s: (off + i,) + (0,) * (v.ndim - 1))


def fin_back(e, ids, x, zn, dz, wg, wo, gt, after=()):
    x4 = pl.BlockSpec((4, HR, RB, TILE), lambda i, s: (0, 0, e * (HR // RB) + i, 0))
    xs = pl.BlockSpec((HALF, RB, N), lambda i, s: (0, i, 0))
    ps = pl.BlockSpec((HALF, RB, TILE), lambda i, s: (0, i, 0))
    dgs = pl.BlockSpec((RB, N, CH), lambda i, s: (i, 0, 0))
    acc = full((CH, CH))
    return call(finb_kernel, (HR // RB,), [x4] * 4 + [part_spec(zn, e), part_spec(dz, e), acc, acc, full((CH, 2))]
                + [pl.BlockSpec(memory_space=pl.ANY)] * len(after),
                [dgs, xs, xs] + [ps] * DEV + [acc] * 3,
                [sds((HR, N, CH), BF16)] + [sds((HALF, HR, N), BF16)] * 2 + [sds((HALF, HR, TILE), BF16)] * DEV
                + [sds((CH, CH), F32)] * 3,
                [pltpu.VMEM((2, 4, RB * STRIDE, TILE), F32)], prefetch=1, flops=BIG)(
                    ids, *x, zn, dz, wg, wo, gt, *after)


def projb_kernel(form, id_ref, *refs):
    n = 2 if form == 'out' else 8
    da, db = refs[:n], refs[n:2 * n]
    zn_ref, z_ref, dz_ref, dg_ref, m_ref, w_ref, wg_ref, g_ref = refs[2 * n:2 * n + DEV]
    o_ref, dw_ref, dwg_ref, dga_ref, dbi_ref, sa, sb = refs[-7:]
    q = id_ref[0]

    @pl.when(pl.program_id(0) == 0)
    def _():
        for ref in (dw_ref, dwg_ref, dga_ref, dbi_ref):
            ref[...] = jnp.zeros_like(ref)

    def chan(c):
        base = pl.multiple_of(c * PAD, 8)
        for src, dst in ((da, sa), (db, sb)):
            for s in range(n):
                if form == 'out':
                    for l in range(4):
                        dst[s, l, pl.ds(base, RB), :] = src[s][c, :, l * TILE:(l + 1) * TILE].astype(F32)
                else:
                    dst[s & 1, q ^ (s >> 1), pl.ds(base, RB), :] = src[s][c].astype(F32)

    loop(HALF, chan, 2)

    def row(r):
        zn = zn_ref[r]
        m = m_ref[pl.ds(r, 1), :]
        dg = dg_ref[r]
        dzn = nt(dg, wg_ref[...])
        dwg_ref[...] += tn(zn, dg)
        for e in range(2):
            w = w_ref[e * 256:(e + 1) * 256, :]
            p = nt(w, zn)
            parts = []
            for k, src in enumerate((sa, sb)):
                d = jnp.concatenate([src[e, l, pl.ds(r, HALF, stride=PAD), :] for l in range(4)], axis=1) * m
                lin = p[k * TILE:k * TILE + 64]
                sig = sigmoid(p[k * TILE + 64:k * TILE + TILE])
                ds = d * sig
                parts += [ds.astype(BF16), (ds * lin * (1.0 - sig)).astype(BF16)]
            cat = jnp.concatenate(parts, axis=0)
            dzn += tn(cat, w)
            dw_ref[e * 256:(e + 1) * 256, :] += nn(cat, zn)
        dn = dzn.astype(BF16).astype(F32)
        z = z_ref[r]
        mean = jnp.mean(z, axis=-1, keepdims=True)
        cen = z - mean
        rstd = lax.rsqrt(jnp.mean(cen * cen, axis=-1, keepdims=True) + LN_EPS)
        zhat = cen * rstd
        dga_ref[...] += jnp.sum((dn * zhat).reshape(N // 8, 8, CH), axis=0)
        dbi_ref[...] += jnp.sum(dn.reshape(N // 8, 8, CH), axis=0)
        dh = dn * g_ref[0:1]
        m1 = jnp.mean(dh, axis=-1, keepdims=True)
        m2 = jnp.mean(dh * zhat, axis=-1, keepdims=True)
        o_ref[r] = dz_ref[r] + rstd * (dh - m1 - zhat * m2)

    loop(RB, row, 2)


def proj_back(form, e, ids, da, db, zn, z, dz, dg, mask, w, wg, g, prev=None, after=()):
    off = e * (HR // RB)
    if form == 'out':
        ps = pl.BlockSpec((HALF, RB, N), lambda i, s: (0, off + i, 0))
        o_spec, o_rows = part_spec(z, e), ROWS
    else:
        ps = pl.BlockSpec((HALF, RB, TILE), lambda i, s: (0, i, 0))
        o_spec, o_rows = pl.BlockSpec((RB, N, CH), lambda i, s: (i, 0, 0)), HR
    rows = [zn, z, dz, dg, mask]
    in_specs, args, aliases = chained(
        [ps] * (2 * len(da)) + [part_spec(v, e) for v in rows] + [full((512, CH)), full((CH, CH)), full((2, CH))],
        [*da, *db, *rows, w, wg, g], prev, 0)
    return call(functools.partial(projb_kernel, form), (HR // RB,),
                in_specs + [pl.BlockSpec(memory_space=pl.ANY)] * len(after),
                [o_spec, full((512, CH)), full((CH, CH)), full((DEV, CH)), full((DEV, CH))],
                [sds((o_rows, N, CH), F32), sds((512, CH), F32), sds((CH, CH), F32), sds((DEV, CH), F32),
                 sds((DEV, CH), F32)],
                [pltpu.VMEM((2, 4, HALF * PAD, TILE), F32)] * 2, prefetch=1,
                aliases={k + 1: v for k, v in aliases.items()}, flops=2 * BIG)(
                    ids, *args, *after)


def solution(mesh):
    row_spec = P(('data', 'dap'))
    grad_spec = P('data')

    def xor(v, s):
        if s == 0:
            return v
        return lax.ppermute(v, 'dap', [(i, i ^ s) for i in range(DEV)])

    def device_body(pair_act, pair_mask, grad_out, ln_pair, w_in, ln_tri, w_out):
        idx = lax.axis_index('dap').astype(jnp.int32)
        h = lax.rem(idx, 2)
        ids = jnp.stack([idx // 2, h])
        mask = pair_mask.astype(F32)
        masks = [xor(mask, s) for s in range(DEV)]
        g_pair = ln_pair.astype(F32)
        g_tri = ln_tri.astype(F32)

        def rel(v, axis=0):
            lo, hi = jnp.split(v, 2, axis=axis)
            return jnp.where(h == 0, v, jnp.concatenate([hi, lo], axis=axis))

        w_rel, wg, wo_rel, gt_rel = [], [], [], []
        for u in range(2):
            wt = w_in[u, :, :512].T.reshape(4, 2, HALF, CH).transpose(1, 0, 2, 3).reshape(512, CH)
            w_rel.append(rel(wt))
            wg.append(w_in[u, :, 512:])
            wo_rel.append(rel(w_out[u]))
            gt_rel.append(rel(g_tri[u].T))

        def spread(v):
            return [v] + [xor(v, s) for s in HOPS]

        def gather_proj(parts, u):
            w = w_rel[u][:256]
            prev = proj_chunk(ids, 0, 2, [v for part in parts for v in part[:2]], masks, w, 0, None)
            far = []
            for t, (_, _, r2, r4) in enumerate(parts):
                far.append(xor(r4, 2) if t % 2 else xor(r2, 4))
                near = [r2, xor(r2, 1), r4, xor(r4, 1)]
                prev = proj_chunk(ids, 2, 4, near, masks, w, t, prev)
            for t in range(0, NCH, 2):
                pairs = []
                for i in (t, t + 1):
                    pairs += [far[i], xor(far[i], 1)]
                prev = proj_chunk(ids, 6, 2, pairs, masks, w, t, prev)
            return prev

        def triangle(form, a, b):
            keep, send, dep = [], [], ()
            for part in range(2):
                k, v = tri_forward(form, part, ids, a, b, dep)
                keep, send, dep = keep + [k], send + [xor(v, 1)], (k,)
            return keep + send

        parts, prev = [], None
        for t in range(NCH):
            chunk, zn0 = ln_chunk(pair_act, g_pair[0], t, prev)
            parts, prev = parts + [spread(chunk)], [zn0]
        a0, b0 = gather_proj(parts, 0)
        x0 = triangle('out', a0, b0)
        parts, prev = [], None
        for t in range(NCH):
            chunk, z1, zn1 = fin_chunk(x0, pair_act, zn0, wg[0], wo_rel[0], gt_rel[0], g_pair[1], t, prev)
            parts, prev = parts + [spread(chunk)], [z1, zn1]
        a1, b1 = gather_proj(parts, 1)
        x1 = triangle('in', a1, b1)

        def exchange(pieces):
            return [xor(v, s) for s, v in enumerate(pieces)]

        def split(out):
            dg, dk, ds = out[:3]
            return dg, [dk, xor(ds, 1)], exchange(out[3:11]), out[11:], dk

        fb1 = [split(fin_back(0, ids, x1, zn1, grad_out, wg[1], wo_rel[1], gt_rel[1]))]
        out = fin_back(1, ids, x1, zn1, grad_out, wg[1], wo_rel[1], gt_rel[1], (fb1[0][4],))
        fb1 += [split(out)]
        dx1, dp1 = fb1[0][1] + fb1[1][1], fb1[0][2] + fb1[1][2]
        da, db, last = [], [], fb1[1][4]
        for e in range(2):
            out = tri_back('da_in', ids, b1, dx1, e, (last,))
            da.append(exchange(out))
            out = tri_back('db_in', ids, a1, dp1, e, (out[0],))
            db.append(exchange(out))
            last = out[0]
        pb1, fb0 = [], []
        for e in range(2):
            pb1.append(proj_back('in', e, ids, da[e], db[e], zn1, z1, grad_out, fb1[e][0], mask, w_rel[1], wg[1],
                                 g_pair[1], after=(last,)))
            fb0.append(split(fin_back(e, ids, x0, zn0, pb1[e][0], wg[0], wo_rel[0], gt_rel[0])))
            last = fb0[e][4]
        da_k, da_s = tri_back('da_out', ids, b0, fb0[0][1] + fb0[1][1])
        da_0 = [da_k, xor(da_s, 1)]
        db_k, db_s = tri_back('db_out', ids, a0, fb0[0][2] + fb0[1][2], after=(da_k,))
        db_0 = [db_k, xor(db_s, 1)]
        pb0, prev = [], None
        for e in range(2):
            pb0.append(proj_back('out', e, ids, da_0, db_0, zn0, pair_act, pb1[e][0], fb0[e][0], mask, w_rel[0],
                                 wg[0], g_pair[0], prev=prev))
            prev = [pb0[e][0]]

        def fin_grads(fb):
            dwo, dga, dbi = [fb[0][3][i] + fb[1][3][i] for i in range(3)]
            return rel(dwo), jnp.stack([jnp.sum(rel(dga), 1), jnp.sum(rel(dbi), 1)])

        def proj_grads(one, two):
            dw, dwg, dgp, dbp = [v + w for v, w in zip(one, two)]
            return [rel(dw).reshape(2, 4, HALF, CH).transpose(1, 0, 2, 3).reshape(512, CH), dwg, dgp, dbp]

        def total(parts):
            v = jnp.concatenate(parts, axis=0)
            for s in HOPS:
                v = v + xor(v, s)
            cuts = []
            for part in parts:
                cuts.append(part.shape[0] + (cuts[-1] if cuts else 0))
            return jnp.split(v, cuts[:-1])

        def ln_grad(dgp, dbp):
            return jnp.stack([jnp.sum(dgp, 0), jnp.sum(dbp, 0)])

        (dwo_0, tri_0), (dwo_1, tri_1) = fin_grads(fb0), fin_grads(fb1)
        early = total(proj_grads(pb1[0][1:], pb1[1][1:]) + [dwo_1, dwo_0, tri_1, tri_0])
        early, one, two = lax.optimization_barrier((early, pb0[0][1:], pb0[1][1:]))
        dw_1, dwg_1, dgp_1, dbp_1, dwo_1, dwo_0, tri_1, tri_0 = early
        dw_0, dwg_0, dgp_0, dbp_0 = total(proj_grads(one, two))
        return (pb0[1][0], jnp.stack([ln_grad(dgp_0, dbp_0), ln_grad(dgp_1, dbp_1)]),
                jnp.stack([jnp.concatenate([dw_0.T, dwg_0], axis=1), jnp.concatenate([dw_1.T, dwg_1], axis=1)]),
                jnp.stack([tri_0, tri_1]), jnp.stack([dwo_0, dwo_1]))


    return jax.shard_map(device_body, mesh=mesh,
                         in_specs=(row_spec, row_spec, row_spec, P(), P(), P(), P()),
                         out_specs=(row_spec, grad_spec, grad_spec, grad_spec, grad_spec),
                         check_vma=False)
```
